256 devices in a mesh: groups: 2 (over y), dp: 2 (over core), tensor: 64 (over x, z).
Axes of the slice: x: 4, y: 2, z: 16, core: 2. Of those that a mesh axis runs over, the one named last changes fastest.
The devices are a block of a 4x16x16 slice.
Arguments:
- hidden_in: bfloat16 [4, 1024, 5120], P(('groups', 'dp'), 'tensor'), parts along dimension 0, may hold values from -40 to 40
- first_values: bfloat16 [4, 1024, 8192], P(('groups', 'dp'), 'tensor'), parts along dimension 0, may hold values from -6 to 6
- qkv_weight: bfloat16 [5120, 3, 8192], P(None, None, 'tensor'), may hold values from -1 to 1
- out_weight: bfloat16 [8192, 5120], P('tensor'), may hold values from -0.1875 to 0.1875
- mix_table: float32 [8, 2], replicated, may hold values from 0.2 to 1
- mix_index: int32 [64], P('tensor'), may hold values from 0 to 7
- lengths: int32 [4], P(('groups', 'dp')), parts along dimension 0, may hold values from 256 to 1024
Outputs:
- attn_out: bfloat16 [4, 1024, 5120], P(('groups', 'dp'), 'tensor'), parts along dimension 0
The draws below stay inside these ranges and needn't reach their ends.
There are 2 independent parts, one for each index of `groups`. The reference program is written for one: setup_inputs(seed, part) draws one part's arguments, and reference() takes and returns one part's arrays. A program takes and returns all parts, laid end to end along the dimension named above; an argument that names none is the same for every part. Nothing has to cross between parts.
All inputs are finite; a program needn't handle non-finite values.
Results may differ from the reference program's by a relative error of at most 0.0077.
Values may be sent and summed in bfloat16 or wider, within the bound.
No kernel may reach another device: no remote copies, remote signals or barrier semaphores. Data moves between devices by JAX's collectives and lax.ppermute only.
A program may use at most 128 MiB of HBM per device.

```python
import math
import jax
import jax.numpy as jnp
from jax import lax

D = 5120
HS = 128
MIXES = 8
SEQ = 1024
HEADS = 64
SEQS = 2


def draw_hidden_in(key, part):
    samples = jnp.clip(jax.random.normal(jax.random.fold_in(key, 11), (SEQS, SEQ, D), jnp.float32), -6.0, 6.0)
    return samples.astype(jnp.bfloat16)


def draw_qkv_weight(key, part):
    inner_width = HEADS * HS
    spread = 1.0 / math.sqrt(D)
    weights = jax.random.normal(jax.random.fold_in(key, 21), (D, 3, inner_width), jnp.float32) * spread
    return jnp.clip(weights, -1.0, 1.0).astype(jnp.bfloat16)


def with_ends(drawn, own_key, least, top_value):
    longest = drawn.shape.index(max(drawn.shape))
    spots = []
    for shift in (0, 1):
        where = [jax.random.randint(jax.random.fold_in(own_key, axis), (), 0, length) for axis, length in enumerate(drawn.shape)]
        where[longest] = (where[longest] + shift) % drawn.shape[longest]
        spots.append(tuple(where))
    return drawn.at[spots[0]].set(least).at[spots[1]].set(top_value)


def level_of(key, dims, cuts, smallest, high):
    gain, own = 1.0, jax.random.fold_in(key, 6)
    for position, shards_of in cuts:
        steps = jnp.exp(jax.random.uniform(jax.random.fold_in(own, position), (shards_of,), jnp.float32, smallest / len(cuts), high / len(cuts)))
        gain = gain * jnp.repeat(steps, dims[position] // shards_of).reshape([-1 if axis == position else 1 for axis in range(len(dims))])
    return gain


def scatter_about(stream_key, dims, width, limit, shards=(), kind=jnp.bfloat16):
    values = width * jax.random.normal(stream_key, dims, jnp.float32)
    if shards:
        values = values * level_of(stream_key, dims, shards, -0.22, 0.18)
    return jnp.clip(values, -limit, limit).astype(kind)


def setup_inputs(seed: int = 0, part: int = 0) -> dict:
    splits = jax.random.split(jax.random.key(seed), 8)
    own_keys = jax.random.split(jax.random.fold_in(splits[7], part), 8)
    hidden_in = draw_hidden_in(jax.random.fold_in(jax.random.fold_in(splits[7], part), 71), part)
    first_values = scatter_about(own_keys[1], (SEQS, SEQ, HEADS * HS), 1.0, 6.0, ((0, 2), (1, 64)))
    qkv_weight = draw_qkv_weight(jax.random.fold_in(splits[7], 71), part)
    out_weight = scatter_about(splits[3], (HEADS * HS, D), (8 * HS) ** -0.5, 0.1875, ((0, 64),))
    mix_table = jnp.clip(jax.random.uniform(splits[4], (MIXES, 2), jnp.float32, 0.2, 1.0), 0.2, 1.0)
    mix_index = with_ends(jax.random.randint(splits[5], (HEADS,), 0, MIXES), jax.random.fold_in(splits[5], 1), 0, MIXES - 1).astype(jnp.int32)
    lengths = jax.random.randint(own_keys[6], (SEQS,), SEQ // 4, SEQ + 1).astype(jnp.int32)
    return {"hidden_in": hidden_in, "first_values": first_values, "qkv_weight": qkv_weight, "out_weight": out_weight, "mix_table": mix_table, "mix_index": mix_index, "lengths": lengths}


NEG_FILL = -1e+30

def reference(hidden_in, first_values, qkv_weight, out_weight, mix_table, mix_index, lengths):
    merged_weight = qkv_weight.reshape(D, 3 * HEADS * HS)
    lambdas = mix_table[mix_index]
    score_scale = 1.0 / math.sqrt(HS)
    positions = jnp.arange(SEQ, dtype=jnp.int32)

    def one_sequence(packed):
        tok_rows, firsts, valid_length = packed
        projected = jnp.dot(tok_rows, merged_weight, preferred_element_type=jnp.float32).astype(jnp.bfloat16)
        split_parts = projected.reshape(SEQ, 3, HEADS, HS)
        first_float = firsts.reshape(SEQ, HEADS, HS).astype(jnp.float32)
        value_float = split_parts[:, 2].astype(jnp.float32)
        mixed_values = (lambdas[None, :, 0:1] * value_float + lambdas[None, :, 1:2] * first_float).astype(jnp.bfloat16)
        allowed = (positions[None, :] <= positions[:, None]) & (positions[None, :] < valid_length)

        def one_head(items):
            query_rows, key_rows, value_rows = items
            scores = jnp.dot(query_rows, key_rows.T, preferred_element_type=jnp.float32) * score_scale
            scores = jnp.where(allowed, scores, NEG_FILL)
            row_max = lax.optimization_barrier(jnp.max(scores, axis=1, keepdims=True))
            raised = jnp.exp(scores - row_max)
            weights = (raised / lax.optimization_barrier(jnp.sum(raised, axis=1, keepdims=True))).astype(jnp.bfloat16)
            return jnp.dot(weights, value_rows, preferred_element_type=jnp.float32).astype(jnp.bfloat16)
        per_head = lax.map(one_head, (jnp.transpose(split_parts[:, 0], (1, 0, 2)), jnp.transpose(split_parts[:, 1], (1, 0, 2)), jnp.transpose(mixed_values, (1, 0, 2))))
        attended = jnp.transpose(per_head, (1, 0, 2)).reshape(SEQ, HEADS * HS)
        return jnp.dot(attended, out_weight, preferred_element_type=jnp.float32).astype(jnp.bfloat16)
    return lax.map(one_sequence, (hidden_in, first_values, lengths))
```

```python
import functools
import math

import jax
import jax.numpy as jnp
from jax import lax
from jax.experimental import pallas as pl
from jax.experimental.pallas import tpu as pltpu
from jax.sharding import Mesh
from jax.sharding import PartitionSpec as P

TENSOR = ("tensor_0", "tensor_1")
COLS, RING, CORE = "tensor_0", "tensor_1", "dp"

NEG_FILL = -1e30


def shifted(value, axis, step):
    size = lax.axis_size(axis)
    return lax.ppermute(value, axis, [(i, (i + step) % size) for i in range(size)])


def swapped(value):
    return shifted(value, CORE, 1)


def own_half(value, axis):
    half = value.shape[axis] // 2
    return lax.dynamic_slice_in_dim(value, lax.axis_index(CORE) * half, half, axis)


def together(values, *others):
    return lax.optimization_barrier(tuple(values) + others)[: len(values)]


def first_part(value, axis):
    return lax.slice_in_dim(value, 0, value.shape[axis] // 2, axis=axis)


def second_part(value, axis):
    return lax.slice_in_dim(value, value.shape[axis] // 2, value.shape[axis], axis=axis)


SMEM = pl.BlockSpec(memory_space=pltpu.SMEM)
VMEM = pl.BlockSpec(memory_space=pltpu.VMEM)
MIB = 1024 * 1024


def limits(size):
    return pltpu.CompilerParams(vmem_limit_bytes=size * MIB)


def project_kernel(heads, place_ref, rows_ref, firsts_ref, *refs):
    *piece_refs, out_ref = refs
    core, column, shift = place_ref[0], place_ref[1], heads
    half = rows_ref.shape[1] // 2
    depth = half // 2
    width = out_ref.shape[2]
    total = None
    for quarter in range(4):
        if len(piece_refs) == 1:
            base = quarter * depth
            weight = [piece_refs[0][kind, base : base + depth, :] for kind in range(3)]
            left = rows_ref[:, base : base + depth]
        else:
            side = core if quarter < 2 else 1 - core
            base = pl.multiple_of(side * half + quarter % 2 * depth, 128)
            weight = [piece_refs[quarter][kind] for kind in range(3)]
            left = rows_ref[:, pl.ds(base, depth)]
        part = jnp.dot(
            left, jnp.concatenate(weight, axis=1), preferred_element_type=jnp.float32
        )
        total = part if total is None else total + part
    for kind in range(3):
        out_ref[kind] = total[:, kind * width : (kind + 1) * width].astype(out_ref.dtype)
    columns = firsts_ref.shape[1]
    head = lax.rem(column + shift + columns, columns)
    out_ref[3] = firsts_ref[:, head].reshape(out_ref.shape[1:])


def project(shift, place, rows, firsts, *pieces):
    width = pieces[0].shape[2]
    return pl.pallas_call(
        functools.partial(project_kernel, shift),
        in_specs=[SMEM] + [VMEM] * (2 + len(pieces)),
        out_specs=VMEM,
        out_shape=jax.ShapeDtypeStruct((4, rows.shape[0], width), jnp.bfloat16),
        compiler_params=limits(20),
        name="project",
    )(place, rows, firsts, *pieces)


OFFSETS = (0, 1, -1, 2)


def attend_kernel(scale, ring, place_ref, length_ref, index_ref, mix_ref, *refs):
    block_refs, out_refs, mixed_ref = refs[:4], refs[4:8], refs[8]
    _, block_rows, width = block_refs[0].shape
    columns = len(block_refs)
    column, place = place_ref[1], place_ref[2]
    rows_here = block_rows // ring
    bases = [lax.rem(column - d + columns, columns) * block_rows for d in OFFSETS]

    def inside(shape, axis):
        spot = lax.broadcasted_iota(jnp.int32, shape, axis) + place * rows_here
        return jnp.where(spot >= block_rows, spot - block_rows, spot)

    own, first = mix_ref[index_ref[0], 0], mix_ref[index_ref[0], 1]
    for index, block in enumerate(block_refs):

        @pl.loop(0, ring)
        def _(chunk):
            source = pl.multiple_of(lax.rem(place + chunk, ring) * rows_here, rows_here)
            here = pl.multiple_of(chunk * rows_here, rows_here)
            value = block[2, pl.ds(here, rows_here), :].astype(jnp.float32)
            early = block[3, pl.ds(source, rows_here), :]
            mixed_ref[pl.ds(index * block_rows + here, rows_here), :] = (
                own * value + first * early.astype(jnp.float32)
            ).astype(jnp.bfloat16)

    keys = jnp.concatenate([block[1] for block in block_refs], axis=0)
    lane_spots = inside((1, block_rows), 1)
    key_positions = jnp.concatenate([base + lane_spots for base in bases], axis=1)
    usable = key_positions < length_ref[0]
    row_spots = inside((block_rows, 1), 0)
    for index, block in enumerate(block_refs):
        scores = (
            lax.dot_general(
                block[0], keys, (((1,), (1,)), ((), ())), preferred_element_type=jnp.float32
            )
            * scale
        )
        allowed = (key_positions <= bases[index] + row_spots) & usable
        scores = jnp.where(allowed, scores, NEG_FILL)
        raised = jnp.exp(scores - jnp.max(scores, axis=1, keepdims=True))
        weights = (raised / jnp.sum(raised, axis=1, keepdims=True)).astype(jnp.bfloat16)
        out_refs[index][...] = jnp.dot(
            weights, mixed_ref[...], preferred_element_type=jnp.float32
        ).astype(jnp.bfloat16)


def attend(place, length, index, mix_table, blocks):
    _, block_rows, width = blocks[0].shape
    return pl.pallas_call(
        functools.partial(attend_kernel, 1.0 / math.sqrt(width), lax.axis_size(RING)),
        in_specs=[SMEM] * 4 + [VMEM] * 4,
        out_specs=[VMEM] * 4,
        out_shape=[jax.ShapeDtypeStruct((block_rows, width), jnp.bfloat16)] * len(blocks),
        scratch_shapes=[pltpu.VMEM((len(blocks) * block_rows, width), jnp.bfloat16)],
        compiler_params=limits(20),
        name="attend",
    )(place, length, index, mix_table, *blocks)


def output_kernel(step, place_ref, *refs):
    inputs, whole, mine_refs, other_refs = refs[:4], refs[4], refs[5:9], refs[9:13]
    out_ref, up_ref, down_ref = refs[13:16]
    left = jnp.concatenate([ref[...] for ref in inputs], axis=1)
    chunks, chunk_rows, width = out_ref.shape
    quarter = width // 4
    core = place_ref[0]
    for side, pieces in enumerate((mine_refs, other_refs)):
        ahead, behind, *fars = pieces
        base = (core if side == 0 else 1 - core) * (width // 2)
        for part, far in enumerate(fars):

            @pl.loop(0, quarter // step)
            def _(index):
                start = pl.multiple_of(index * step, 128)
                near = pl.ds(pl.multiple_of(part * quarter + start, 128), step)
                spot = pl.ds(pl.multiple_of(base + part * quarter + start, 128), step)
                weight = jnp.concatenate(
                    [whole[:, spot], ahead[:, near], behind[:, near], far[:, pl.ds(start, step)]],
                    axis=0,
                )
                result = jnp.dot(left, weight, preferred_element_type=jnp.float32)
                out_ref[:, :, spot] = result.reshape(chunks, chunk_rows, step)
                middle = chunks // 2 * chunk_rows
                up_ref[:, spot] = result[middle : middle + chunk_rows].astype(up_ref.dtype)
                down_ref[:, spot] = result[middle + chunk_rows : middle + 2 * chunk_rows].astype(
                    down_ref.dtype
                )


def output_parts(place, inputs, whole, mine, other, chunks):
    rows, width = inputs[0].shape[0], whole.shape[1]
    quarter = width // 4
    step = 256 if quarter % 256 == 0 else 128
    chunk = (rows // chunks, width)
    return pl.pallas_call(
        functools.partial(output_kernel, step),
        in_specs=[SMEM] + [VMEM] * 13,
        out_specs=[VMEM] * 3,
        out_shape=[
            jax.ShapeDtypeStruct((chunks,) + chunk, jnp.float32),
            jax.ShapeDtypeStruct(chunk, jnp.bfloat16),
            jax.ShapeDtypeStruct(chunk, jnp.bfloat16),
        ],
        compiler_params=limits(24),
        name="output",
    )(place, *inputs, whole, *mine, *other)


def ring_gather(chunk, meanwhile):
    size = lax.axis_size(RING)
    ups, downs = [], []
    up = down = chunk
    for step in range(size // 2):
        waits = meanwhile(step)
        if waits:
            (up,) = together((up,), *waits)
        up = shifted(up, RING, -1)
        ups.append(up)
        if step < size // 2 - 1:
            down = shifted(down, RING, 1)
            downs.append(down)
    return jnp.concatenate([chunk] + ups + downs[::-1], axis=0)


def ring_reduce(parts, up, down):
    size = lax.axis_size(RING)
    half = size // 2
    previous = None
    for step in range(half):
        last = step == half - 1
        if step:
            arrived = up
            if previous is not None:
                (up,) = together((up,), previous)
            up = (parts[half - step] + up.astype(jnp.float32)).astype(jnp.bfloat16)
            previous = down
            if not last:
                (down,) = together((down,), arrived)
                down = (parts[half + 1 + step] + down.astype(jnp.float32)).astype(jnp.bfloat16)
        up = shifted(up, RING, 1)
        if not last:
            down = shifted(down, RING, -1)
    return parts[0] + up.astype(jnp.float32) + down.astype(jnp.float32)


def body(hidden_in, first_values, qkv_weight, out_weight, mix_table, mix_index, lengths):
    place = jnp.stack([lax.axis_index(axis) for axis in (CORE, COLS, RING)]).astype(jnp.int32)
    columns, ring = lax.axis_size(COLS), lax.axis_size(RING)
    head_size = qkv_weight.shape[2]

    by_kind = jnp.transpose(qkv_weight, (1, 0, 2))
    quarter = by_kind.shape[1] // 4
    first = lax.axis_index(CORE) * 2 * quarter
    mine_a = lax.dynamic_slice_in_dim(by_kind, first, quarter, 1)
    mine_b = lax.dynamic_slice_in_dim(by_kind, first + quarter, quarter, 1)
    ahead_a, behind_b = shifted(mine_a, COLS, -1), shifted(mine_b, COLS, 1)
    ahead_b, behind_a = shifted(mine_b, COLS, -1), shifted(mine_a, COLS, 1)
    ahead_a, behind_b, ahead_b, behind_a = together((ahead_a, behind_b, ahead_b, behind_a))
    far_a, far_b = shifted(ahead_a, COLS, -1), shifted(behind_b, COLS, 1)
    out_mine = own_half(out_weight, 1)
    (out_mine,) = together((out_mine,), ahead_a)
    out_ahead, out_behind = shifted(out_mine, COLS, -1), shifted(out_mine, COLS, 1)

    (chunk,) = together((hidden_in[0],), mine_a, mine_b)
    late = {ring // 2 - 2: (ahead_a, behind_b)}
    rows = ring_gather(chunk, lambda step: late.get(step, ()))
    firsts = first_values[0].reshape(-1, columns, ring, head_size).transpose(2, 1, 0, 3)
    firsts = lax.all_to_all(firsts, RING, split_axis=0, concat_axis=0, tiled=True)

    to_ahead = project(
        1, place, rows, firsts, ahead_a, ahead_b, swapped(ahead_a), swapped(ahead_b)
    )
    to_behind = project(
        -1, place, rows, firsts, behind_a, behind_b, swapped(behind_a), swapped(behind_b)
    )
    far_a, far_b = together((far_a, far_b), to_ahead, to_behind)
    to_far = project(2, place, rows, firsts, far_a, far_b, swapped(far_a), swapped(far_b))
    own = project(0, place, rows, firsts, by_kind)
    attended = attend(
        place,
        lengths,
        mix_index,
        mix_table,
        (own, shifted(to_ahead, COLS, 1), shifted(to_behind, COLS, -1), shifted(to_far, COLS, 2)),
    )
    inputs = (
        attended[0],
        shifted(attended[1], COLS, -1),
        shifted(attended[2], COLS, 1),
        shifted(attended[3], COLS, 2),
    )

    out_ahead, out_behind = together((out_ahead, out_behind), attended[1])
    out_far_a = shifted(first_part(out_ahead, 1), COLS, -1)
    out_far_b = shifted(second_part(out_behind, 1), COLS, 1)
    out_pieces = (out_ahead, out_behind, out_far_a, out_far_b)
    others = tuple(swapped(piece) for piece in out_pieces)
    parts = output_parts(place, inputs, out_weight, out_pieces, others, ring)
    return ring_reduce(*parts).astype(jnp.bfloat16)[None]


def solution(mesh):
    torus = Mesh(
        mesh.devices.reshape(mesh.shape["groups"], mesh.shape["dp"], 4, 16),
        ("groups", "dp", "tensor_0", "tensor_1"),
    )
    placed = (
        P(("groups", "dp"), TENSOR, None),
        P(("groups", "dp"), TENSOR, None),
        P(None, None, TENSOR),
        P(TENSOR, None),
        P(),
        P(TENSOR),
        P(("groups", "dp")),
    )
    return jax.shard_map(
        body,
        mesh=torus,
        in_specs=placed,
        out_specs=P(("groups", "dp"), TENSOR, None),
        check_vma=False,
    )
```
